512 devices in a mesh: mem: 32 (over z_hi, y, core), kvh: 4 (over z_lo), row: 4 (over x).
Axes of the slice: x: 4, y: 8, z: 8 (z_hi: 2, z_lo: 4; z = z_hi * 4 + z_lo), core: 2. Of those that a mesh axis runs over, the one named last changes fastest.
Arguments:
- queries: bfloat16 [1024, 8192], P(('mem', 'kvh', 'row')), may hold values from -120 to 120
- output_gradient: bfloat16 [1024, 8192], P(('mem', 'kvh', 'row')), may hold values from -6 to 6
- keys: bfloat16 [24576, 1024], P('mem', 'kvh'), may hold values from -6 to 6
- values: bfloat16 [24576, 1024], P('mem', 'kvh'), may hold values from -6 to 6
- text_video: int32 [128, 8], P(None, 'row'), may hold values from 0 to 95
- video_blocks: int32 [96], replicated, may hold values from 1 to 4, 192 in all
Outputs:
- attention_out: bfloat16 [1024, 8192], P(('mem', 'kvh', 'row'))
- query_grad: bfloat16 [1024, 8192], P(('mem', 'kvh', 'row'))
- keys_gradient: bfloat16 [24576, 1024], P('mem', 'kvh')
- values_gradient: bfloat16 [24576, 1024], P('mem', 'kvh')
The draws below stay inside these ranges and needn't reach their ends.
Inputs may be any that keep to these rules, and one draw needn't show every extreme that they name: Row sees images 0 to text_video. `video_blocks`: they sum to 192.
All inputs are finite; a program needn't handle non-finite values.
Results may differ from the reference program's by a relative error of at most 0.015.
Values may be sent and summed in bfloat16 or wider, within the bound.
A program may use at most 64 MiB of HBM per device.

```python
import math
import jax
import jax.numpy as jnp
import numpy as np
from jax import lax

QUERY_HEADS = 64
KEY_VALUE_HEADS = 8
HEAD_WIDTH = 128
FRAME = 128
ROW_DEV = 2
TEXT_ROW_COUNT = 1024
VISUAL_TOKENS = 24576
BLOCKS = 192
VIDEOS = 96
N_MEM = 32
N_KVH = 4
N_ROW = 4


def drawn_pair(key):
    base_key = jax.random.fold_in(key, 4099)
    key_query, random_key_seeds = jax.random.split(base_key, 2)
    queries = jnp.clip(2.0 * jax.random.normal(key_query, (TEXT_ROW_COUNT, QUERY_HEADS, HEAD_WIDTH), jnp.float32), -12.0, 12.0)
    keys = jnp.clip(jax.random.normal(random_key_seeds, (VISUAL_TOKENS, KEY_VALUE_HEADS, HEAD_WIDTH), jnp.float32), -6.0, 6.0)
    return (queries.reshape(TEXT_ROW_COUNT, QUERY_HEADS * HEAD_WIDTH), keys.reshape(VISUAL_TOKENS, KEY_VALUE_HEADS * HEAD_WIDTH))


def draw_queries(key, part):
    return drawn_pair(key)[0].astype(jnp.bfloat16)


def draw_keys(key, part):
    return drawn_pair(key)[1].astype(jnp.bfloat16)


def plant(values, rng, low, largest):
    dims = values.shape
    index_at = [jax.random.randint(jax.random.fold_in(rng, axis), (), 0, dims[axis]) for axis in range(len(dims))]
    values = values.at[tuple(index_at)].set(low)
    longest = dims.index(max(dims))
    index_at[longest] = (index_at[longest] + 1) % dims[longest]
    return values.at[tuple(index_at)].set(largest)


def shard_levels(stream_key, shape, pieces, low, high):
    def one(position, blocks):
        steps = jax.random.uniform(jax.random.fold_in(jax.random.fold_in(stream_key, 6), position), (blocks,), jnp.float32, low / len(pieces), high / len(pieces))
        return jnp.repeat(jnp.exp(steps), shape[position] // blocks).reshape((-1,) + (1,) * (len(shape) - position - 1))

    loudness = one(*pieces[0])
    for cut in pieces[1:]:
        loudness = loudness * one(*cut)
    return loudness


def profile(number_of, total, bound, slope):
    weights = [(1 << 20) // math.isqrt(rank ** slope) + 1 for rank in range(2, number_of + 1)]
    rest, given = total - bound - (number_of - 1), [1] * (number_of - 1)
    while rest > 0:
        candidates = [i for i in range(number_of - 1) if given[i] < bound]
        mass, remaining = sum([weights[i] for i in candidates]), rest
        for i in candidates:
            extra = min(bound - given[i], max(1, remaining * weights[i] // mass), rest)
            given[i] = given[i] + extra
            rest = rest - extra
    return np.array([bound] + given)


def ragged_sizes(rng, number_of, total, most, lean):
    if number_of == 2:
        one = jax.random.randint(rng, (), max(1, total - most), min(most, total - 1) + 1)
        return jnp.stack([one, total - one])
    lengths = jnp.asarray(profile(number_of, total, most, lean), jnp.int32)
    pairs = (number_of - 1) // 2
    source_of, sink = lengths[1:1 + 2 * pairs:2], lengths[2:2 + 2 * pairs:2]
    margin = jnp.minimum(source_of - 1, most - sink)
    passed = jax.random.randint(jax.random.fold_in(rng, 1), (pairs,), 0, 1 << 20) % (margin + 1)
    lengths = lengths.at[1:1 + 2 * pairs:2].set(source_of - passed).at[2:2 + 2 * pairs:2].set(sink + passed)
    return lengths[jax.random.permutation(jax.random.fold_in(rng, 2), number_of)]


def gaussian(rng, extent, scale, bound, cuts=(), kind=jnp.bfloat16):
    array = jax.random.normal(rng, extent, jnp.float32) * scale
    if len(cuts) > 0:
        array = shard_levels(rng, extent, cuts, -0.22, 0.18) * array
    return jnp.clip(array, min=-bound, max=bound).astype(kind)


def setup_inputs(seed: int = 0) -> dict:
    arg_keys = jax.random.split(jax.random.key(seed), 7)
    return {
        "queries": draw_queries(jax.random.fold_in(arg_keys[6], 71), 0),
        "output_gradient": gaussian(arg_keys[1], (TEXT_ROW_COUNT, QUERY_HEADS * HEAD_WIDTH), 1.0, 6.0, ((0, 512),)),
        "keys": draw_keys(jax.random.fold_in(arg_keys[6], 71), 0),
        "values": gaussian(arg_keys[3], (VISUAL_TOKENS, KEY_VALUE_HEADS * HEAD_WIDTH), 1.0, 6.0, ((0, 32), (1, 4))),
        "text_video": plant(jax.random.randint(arg_keys[4], (N_MEM * N_KVH, N_ROW * ROW_DEV), 0, VIDEOS), jax.random.fold_in(arg_keys[4], 1), 0, VIDEOS - 1).astype(jnp.int32),
        "video_blocks": ragged_sizes(arg_keys[5], VIDEOS, BLOCKS, 4, 2).astype(jnp.int32),
    }


masked_score = -1.0e30


def video_of_block(video_blocks, block_count):
    block_ends = jnp.cumsum(video_blocks)
    blocks = jnp.arange(block_count, dtype=jnp.int32)
    return jnp.sum((block_ends[None, :] <= blocks[:, None]).astype(jnp.int32), axis=1)


def one_head(query, gradient, key_head, value_head, visible):
    inverse_root = HEAD_WIDTH ** -0.5
    scores = jnp.dot(query, key_head.T, preferred_element_type=jnp.float32) * inverse_root
    scores = jnp.where(visible, scores, masked_score)
    row_top = jnp.max(scores, axis=1, keepdims=True)
    weight = jnp.where(visible, jnp.exp(scores - row_top), 0.0)
    totals = jnp.sum(weight, axis=1, keepdims=True)
    attention = jnp.dot(weight.astype(jnp.bfloat16), value_head, preferred_element_type=jnp.float32) / totals
    log_mass = row_top + jnp.log(totals)
    probability = jnp.where(visible, jnp.exp(scores - log_mass), 0.0)
    delta = jnp.sum(gradient.astype(jnp.float32) * attention, axis=1, keepdims=True)
    prob_grad = jnp.dot(gradient, value_head.T, preferred_element_type=jnp.float32)
    score_grad = (probability * (prob_grad - delta)).astype(jnp.bfloat16)
    query_grad = jnp.dot(score_grad, key_head, preferred_element_type=jnp.float32) * inverse_root
    keys_gradient = jnp.dot(score_grad.T, query, preferred_element_type=jnp.float32) * inverse_root
    values_gradient = jnp.dot(probability.astype(jnp.bfloat16).T, gradient, preferred_element_type=jnp.float32)
    return attention, query_grad, keys_gradient, values_gradient


def reference(queries, output_gradient, keys, values, text_video, video_blocks):
    key_video = jnp.repeat(video_of_block(video_blocks, VISUAL_TOKENS // FRAME), FRAME)
    visible = key_video[None, :] <= text_video.reshape(TEXT_ROW_COUNT)[:, None]
    heads_per_group = QUERY_HEADS // KEY_VALUE_HEADS
    query_pieces = queries.reshape(TEXT_ROW_COUNT, KEY_VALUE_HEADS, heads_per_group, HEAD_WIDTH).transpose(1, 2, 0, 3)
    gradient_pieces = output_gradient.reshape(TEXT_ROW_COUNT, KEY_VALUE_HEADS, heads_per_group, HEAD_WIDTH).transpose(1, 2, 0, 3)
    key_pieces = keys.reshape(VISUAL_TOKENS, KEY_VALUE_HEADS, HEAD_WIDTH).transpose(1, 0, 2)
    value_pieces = values.reshape(VISUAL_TOKENS, KEY_VALUE_HEADS, HEAD_WIDTH).transpose(1, 0, 2)

    def per_key_head(inputs):
        query_group, grad_group, key_head, value_head = inputs

        def per_query_head(pair_in):
            return one_head(pair_in[0], pair_in[1], key_head, value_head, visible)

        attention, query_grad, keys_gradient, values_gradient = lax.map(per_query_head, (query_group, grad_group))
        return attention, query_grad, jnp.sum(keys_gradient, axis=0), jnp.sum(values_gradient, axis=0)

    attention, query_grad, keys_gradient, values_gradient = lax.map(per_key_head, (query_pieces, gradient_pieces, key_pieces, value_pieces))
    attention_out = attention.transpose(2, 0, 1, 3).reshape(TEXT_ROW_COUNT, QUERY_HEADS * HEAD_WIDTH).astype(jnp.bfloat16)
    query_out = query_grad.transpose(2, 0, 1, 3).reshape(TEXT_ROW_COUNT, QUERY_HEADS * HEAD_WIDTH).astype(jnp.bfloat16)
    keys_result = keys_gradient.transpose(1, 0, 2).reshape(VISUAL_TOKENS, KEY_VALUE_HEADS * HEAD_WIDTH).astype(jnp.bfloat16)
    values_result = values_gradient.transpose(1, 0, 2).reshape(VISUAL_TOKENS, KEY_VALUE_HEADS * HEAD_WIDTH).astype(jnp.bfloat16)
    return (attention_out, query_out, keys_result, values_result)
```

```python
import functools

import jax
import jax.numpy as jnp
from jax import lax
from jax.experimental import pallas as pl
from jax.experimental.pallas import tpu as pltpu
from jax.sharding import PartitionSpec as P

HEADS = 64
KV = 8
D = 128
GROUP = HEADS // KV
ROWS = 2
NY = 8
NZH = 2
NK = 4
NC = 2
NX = 4
COL = NZH * NK * NC
CHIPS = NZH * NY
PIECE = ROWS * GROUP
CH = COL * PIECE
TOK = 768
TOKENS = NC * TOK
TB = 256
NB = TOKENS // TB
QT = TOKENS // NX
FRAME = 128
SCALE = D ** (-0.5)
LOG2E = 1.4426950408889634
CS = SCALE * LOG2E
NEG = -1e30
MESH = pl.DeviceIdType.MESH
BF = jnp.bfloat16
F32 = jnp.float32


def dot_nt(a, b):
    return lax.dot_general(a, b, (((1,), (1,)), ((), ())), preferred_element_type=F32)


def dot_nn(a, b):
    return lax.dot_general(a, b, (((1,), (0,)), ((), ())), preferred_element_type=F32)


def kernel(
    xin, keys, values, nvis,
    fin, kvout,
    buf, kbuf, vbuf, kt, vt, wbuf, dpbuf, mst, stats,
    osend, orecv, dqsend, dqrecv, dk, dv, rssend, rsrecv, agsrc, fsend, frecv,
    a_send, a_recv, kv_send, kv_recv, kv_loc, r_send, r_recv, o_send, o_recv, q_send, q_recv,
    s_send, s_recv, rs_send, rs_recv, f_send, f_recv, ag_send, ag_recv,
):
    m = lax.axis_index("mem")
    k = lax.axis_index("kvh")
    x = lax.axis_index("row")
    c = lax.rem(m, 2)
    n = lax.div(m, 2)
    y = lax.rem(n, NY)
    zh = lax.div(n, NY)
    s = (zh * NK + k) * NC + c

    def column(t):
        zz = lax.div(t, 2)
        return ((lax.div(zz, NK) * NY + y) * 2 + lax.rem(t, 2), lax.rem(zz, NK), x)

    def chip(t):
        return (t * 2 + c, k, x)

    def at_y(t):
        return ((zh * NY + t) * 2 + c, k, x)

    def at_x(t, core):
        return (n * 2 + core, k, t)

    def remote(src, dst, ss, rs, dev):
        return pltpu.make_async_remote_copy(
            src_ref=src, dst_ref=dst, send_sem=ss, recv_sem=rs, device_id=dev, device_id_type=MESH
        )

    other = 1 - c
    mine_cols = pl.ds(pl.multiple_of(c * D, D), D)
    other_cols = pl.ds(pl.multiple_of(other * D, D), D)
    loc_k = pltpu.make_async_copy(keys.at[:, mine_cols], kbuf.at[c], kv_loc.at[0])
    loc_v = pltpu.make_async_copy(values.at[:, mine_cols], vbuf.at[c], kv_loc.at[1])
    loc_k.start()
    loc_v.start()

    barrier = pltpu.get_barrier_semaphore()

    def greet_col(j, _):
        pl.semaphore_signal(barrier, inc=1, device_id=column(lax.rem(s + j, COL)), device_id_type=MESH)
        return 0

    def greet_chip(j, _):
        pl.semaphore_signal(barrier, inc=1, device_id=chip(lax.rem(n + j, CHIPS)), device_id_type=MESH)
        return 0

    lax.fori_loop(1, COL, greet_col, 0)
    lax.fori_loop(1, CHIPS, greet_chip, 0)
    for j in range(1, NX):
        for core in range(2):
            pl.semaphore_signal(
                barrier, inc=1, device_id=at_x(lax.rem(x + j, NX), core), device_id_type=MESH
            )
    pl.semaphore_wait(barrier, (COL - 1) + (CHIPS - 1) + 2 * (NX - 1))

    def a_copy(src_s, dst_s, dev):
        return remote(
            xin.at[lax.rem(dst_s, KV)], buf.at[y, :, src_s], a_send.at[dst_s], a_recv.at[src_s], dev
        )

    def a_start(j, _):
        t = lax.rem(s + j, COL)
        a_copy(s, t, column(t)).start()
        return 0

    lax.fori_loop(1, COL, a_start, 0)
    kcopy = remote(keys.at[:, other_cols], kbuf.at[c], kv_send.at[0], kv_recv.at[0], (n * 2 + other, k, x))
    vcopy = remote(values.at[:, other_cols], vbuf.at[c], kv_send.at[1], kv_recv.at[1], (n * 2 + other, k, x))
    kcopy.start()
    vcopy.start()
    own = xin[lax.rem(s, KV)]
    buf[y, 0, s] = own[0]
    buf[y, 1, s] = own[1]
    loc_k.wait()
    loc_v.wait()

    def a_wait(j, _):
        t = lax.rem(s + j, COL)
        a_copy(t, s, column(t)).wait_recv()
        return 0

    lax.fori_loop(1, COL, a_wait, 0)

    right = at_y(lax.rem(y + 1, NY))
    left = at_y(lax.rem(y + NY - 1, NY))

    def ring(way, kind, t):
        g = lax.rem(y + NY - t, NY) if way == 0 else lax.rem(y + t, NY)
        ref = buf.at[g, kind]
        return remote(ref, ref, r_send.at[way, kind, t], r_recv.at[way, kind, t], right if way == 0 else left)

    def ring_arrival(way, kind, t):
        g = lax.rem(y + NY - 1 - t, NY) if way == 0 else lax.rem(y + 1 + t, NY)
        ref = buf.at[g, kind]
        return remote(ref, ref, r_send.at[way, kind, t], r_recv.at[way, kind, t], right if way == 0 else left)

    for kind in range(2):
        for way in range(2):
            ring(way, kind, 0).start()

    kcopy.wait_recv()
    vcopy.wait_recv()
    for h in range(2):
        kt[:, h * TOK:(h + 1) * TOK] = kbuf[h].T
        vt[:, h * TOK:(h + 1) * TOK] = vbuf[h].T

    def chunk_at(i):
        half = lax.div(i + 1, 2)
        return jnp.where(lax.rem(i, 2) == 1, lax.rem(y + NY - half, NY), lax.rem(y + half, NY))

    def token_block(ref, b):
        h = b * TB // TOK
        return ref[h, b * TB - h * TOK:(b + 1) * TB - h * TOK]

    def forward(i, _):
        @pl.when(lax.rem(i, 2) == 1)
        def _():
            t = lax.div(i - 1, 2)
            for kind in range(2):
                for way in range(2):
                    last_too = kind == way

                    if last_too:
                        ring_arrival(way, kind, t).wait_recv()

                        @pl.when(t < 3)
                        def _():
                            ring(way, kind, t + 1).start()
                    else:
                        @pl.when(t < 3)
                        def _():
                            ring_arrival(way, kind, t).wait_recv()

                        @pl.when(t < 2)
                        def _():
                            ring(way, kind, t + 1).start()

        g = chunk_at(i)
        q = buf[g, 0].reshape(CH, D)
        d = buf[g, 1].reshape(CH, D)
        nv = nvis[g]
        top = jnp.full((1, CH), NEG, F32)
        for b in range(NB):
            sc = dot_nt(token_block(kbuf, b), q)
            wbuf[g, b] = sc
            for u in range(TB // FRAME):
                part = jnp.max(sc[u * FRAME:(u + 1) * FRAME], axis=0, keepdims=True)
                top = jnp.maximum(top, jnp.where(nv > b * (TB // FRAME) + u, part, NEG))
        msc = top * CS
        total = jnp.zeros((1, CH), F32)
        dsum = jnp.zeros((1, CH), F32)
        acc = jnp.zeros((D, CH), F32)
        for b in range(NB):
            dp = dot_nt(token_block(vbuf, b), d)
            dpbuf[g, b] = dp
            ws = []
            for u in range(TB // FRAME):
                bias = jnp.where(nv > b * (TB // FRAME) + u, -msc, NEG)
                ws.append(jnp.exp2(wbuf[g, b, u * FRAME:(u + 1) * FRAME] * CS + bias))
            w = jnp.concatenate(ws, axis=0)
            wbuf[g, b] = w
            total = total + jnp.sum(w, axis=0, keepdims=True)
            dsum = dsum + jnp.sum(w * dp, axis=0, keepdims=True)
            acc = acc + dot_nn(vt[:, b * TB:(b + 1) * TB], w.astype(BF))
        seen = nv > 0
        inv = jnp.where(seen, 1.0 / jnp.where(seen, total, 1.0), 0.0)
        stats[n, g, 0] = jnp.where(seen, msc + jnp.log2(jnp.where(seen, total, 1.0)), NEG)
        stats[n, g, 1] = dsum * inv
        mst[g] = msc
        out = (acc * inv).astype(BF)

        def s_start(j, _):
            t = lax.rem(n + j, CHIPS)
            ref = stats.at[n, g]
            remote(ref, ref, s_send.at[t], s_recv.at[n], chip(t)).start()
            return 0

        lax.fori_loop(1, CHIPS, s_start, 0)

        @pl.when(g == y)
        def _():
            orecv[y] = out

        @pl.when(g != y)
        def _():
            osend[g] = out
            remote(osend.at[g], orecv.at[y], o_send.at[g], o_recv.at[y], at_y(g)).start()

        return 0

    lax.fori_loop(0, NY, forward, 0)

    def s_wait(j, _):
        t = lax.rem(n + j, CHIPS)
        ref = stats.at[t]
        remote(ref, ref, s_send.at[t], s_recv.at[t], chip(t)).wait_recv()
        return 0

    lax.fori_loop(1, CHIPS, s_wait, 0)

    def whole_stats(g):
        peak = stats[0, g, 0]
        for t in range(1, CHIPS):
            peak = jnp.maximum(peak, stats[t, g, 0])
        mass = jnp.zeros((1, CH), F32)
        dsum = jnp.zeros((1, CH), F32)
        for t in range(CHIPS):
            e = jnp.exp2(stats[t, g, 0] - peak)
            mass = mass + e
            dsum = dsum + e * stats[t, g, 1]
        return peak + jnp.log2(mass), dsum / mass

    dk[...] = jnp.zeros_like(dk)
    dv[...] = jnp.zeros_like(dv)

    def backward(i, _):
        g = chunk_at(NY - 1 - i)
        q = buf[g, 0].reshape(CH, D)
        d = buf[g, 1].reshape(CH, D)
        lse, delta = whole_stats(g)
        f = jnp.exp2(mst[g] - lse)
        acc = jnp.zeros((D, CH), F32)
        for b in range(NB):
            p = wbuf[g, b] * f
            ds = (p * (dpbuf[g, b] - delta)).astype(BF)
            rows = slice(b * TB, (b + 1) * TB)
            dv[rows] = dv[rows] + dot_nn(p.astype(BF), d)
            dk[rows] = dk[rows] + dot_nn(ds, q)
            acc = acc + dot_nn(kt[:, rows], ds)
        out = (acc * SCALE).astype(BF)

        @pl.when(g == y)
        def _():
            dqrecv[y] = out

        @pl.when(g != y)
        def _():
            dqsend[g] = out
            remote(dqsend.at[g], dqrecv.at[y], q_send.at[g], q_recv.at[y], at_y(g)).start()

        return 0

    lax.fori_loop(0, NY, backward, 0)

    def rs_copy(src, dst):
        return remote(rssend.at[dst], rsrecv.at[src], rs_send.at[dst], rs_recv.at[src], at_x(dst, c))

    for t in range(NX):
        rssend[t, 0] = (dk[t * QT:(t + 1) * QT] * SCALE).astype(BF)
        rssend[t, 1] = dv[t * QT:(t + 1) * QT].astype(BF)
    for j in (2, 1, 3):
        rs_copy(x, lax.rem(x + j, NX)).start()

    def o_wait(j, _):
        t = lax.rem(y + j, NY)
        remote(osend.at[t], orecv.at[t], o_send.at[t], o_recv.at[t], at_y(t)).wait_recv()
        return 0

    lax.fori_loop(1, NY, o_wait, 0)
    lse, _ = whole_stats(y)
    acc = jnp.zeros((D, CH), F32)
    for t in range(NY):
        acc = acc + orecv[t].astype(F32) * jnp.exp2(stats[zh * NY + t, y, 0] - lse)
    fsend[0] = acc.T.astype(BF).reshape(COL, PIECE, D)

    def q_wait(j, _):
        t = lax.rem(y + j, NY)
        remote(dqsend.at[t], dqrecv.at[t], q_send.at[t], q_recv.at[t], at_y(t)).wait_recv()
        return 0

    lax.fori_loop(1, NY, q_wait, 0)
    acc = jnp.zeros((D, CH), F32)
    for t in range(NY):
        acc = acc + dqrecv[t].astype(F32)
    fsend[1] = acc.T.astype(BF).reshape(COL, PIECE, D)

    def f_copy(src, dst):
        return remote(fsend.at[:, dst], frecv.at[src], f_send.at[dst], f_recv.at[src], column(dst))

    def f_start(j, _):
        f_copy(s, lax.rem(s + j, COL)).start()
        return 0

    lax.fori_loop(1, COL, f_start, 0)
    frecv[s, 0] = fsend[0, s]
    frecv[s, 1] = fsend[1, s]

    for j in range(1, NX):
        rs_copy(lax.rem(x + j, NX), x).wait_recv()
    for a in range(2):
        acc = rssend[x, a].astype(F32)
        for j in range(1, NX):
            acc = acc + rsrecv[lax.rem(x + j, NX), a].astype(F32)
        agsrc[a] = acc.astype(BF)

    core = lax.div(x, 2)
    part = lax.rem(x, 2)

    def ag_copy(t):
        return remote(
            agsrc, kvout.at[:, part, c], ag_send.at[t], ag_recv.at[part, c], at_x(t, core)
        )

    for j in (2, 1, 3):
        ag_copy(lax.rem(x + j, NX)).start()

    @pl.when(core != c)
    def _():
        ag_copy(x).start()

    @pl.when(core == c)
    def _():
        kvout[0, part, c] = agsrc[0]
        kvout[1, part, c] = agsrc[1]

    def f_wait(j, _):
        f_copy(lax.rem(s + j, COL), s).wait_recv()
        return 0

    lax.fori_loop(1, COL, f_wait, 0)
    for h in range(KV):
        for a in range(2):
            fin[a, h] = (frecv[h, a].astype(F32) + frecv[KV + h, a].astype(F32)).astype(BF)

    for pp in range(2):
        for hh in range(2):
            itself = jnp.logical_and(c * 2 + pp == x, hh == c)

            @pl.when(jnp.logical_not(itself))
            def _():
                remote(
                    agsrc, kvout.at[:, pp, hh], ag_send.at[0], ag_recv.at[pp, hh], at_x(x, other)
                ).wait_recv()

    def col_sent(j, _):
        t = lax.rem(s + j, COL)
        a_copy(s, t, column(t)).wait_send()
        f_copy(s, t).wait_send()
        return 0

    lax.fori_loop(1, COL, col_sent, 0)
    kcopy.wait_send()
    vcopy.wait_send()
    for kind in range(2):
        for way in range(2):
            for t in range(4 if kind == way else 3):
                ring(way, kind, t).wait_send()

    def y_sent(j, _):
        t = lax.rem(y + j, NY)
        remote(osend.at[t], orecv.at[y], o_send.at[t], o_recv.at[y], at_y(t)).wait_send()
        remote(dqsend.at[t], dqrecv.at[y], q_send.at[t], q_recv.at[y], at_y(t)).wait_send()
        return 0

    lax.fori_loop(1, NY, y_sent, 0)

    def s_sent(j, _):
        t = lax.rem(n + j, CHIPS)
        ref = stats.at[n]
        remote(ref, ref, s_send.at[t], s_recv.at[n], chip(t)).wait_send()
        return 0

    lax.fori_loop(1, CHIPS, s_sent, 0)
    for j in range(1, NX):
        rs_copy(x, lax.rem(x + j, NX)).wait_send()
        ag_copy(lax.rem(x + j, NX)).wait_send()

    @pl.when(core != c)
    def _():
        ag_copy(x).wait_send()


def per_device(queries, output_gradient, keys, values, text_video, video_blocks):
    n = lax.axis_index("mem") // 2
    both = jnp.stack([queries, output_gradient])
    xin = both.reshape(2, ROWS, KV, GROUP, D).transpose(2, 0, 1, 3, 4).reshape(KV, 2, PIECE, D)
    ids = jnp.arange(video_blocks.shape[0], dtype=jnp.int32)
    ends = jnp.sum(jnp.where(ids <= text_video[..., None], video_blocks, 0), axis=-1)
    frames = TOKENS // FRAME
    seen = jnp.clip(ends - n * frames, 0, frames)
    seen = seen.reshape(NZH, NY, NC, NK, ROWS).transpose(1, 0, 3, 2, 4)
    nvis = jnp.broadcast_to(seen[..., None], (NY, NZH, NK, NC, ROWS, GROUP)).reshape(NY, 1, CH)

    vm = pl.BlockSpec(memory_space=pltpu.VMEM)
    hbm = pl.BlockSpec(memory_space=pl.ANY)
    dma = pltpu.SemaphoreType.DMA
    fin, kvout = pl.pallas_call(
        kernel,
        name="attention_step",
        out_shape=(
            jax.ShapeDtypeStruct((2, KV, PIECE, D), BF),
            jax.ShapeDtypeStruct((2, 2, 2, QT, D), BF),
        ),
        in_specs=[vm, hbm, hbm, vm],
        out_specs=(vm, vm),
        scratch_shapes=[
            pltpu.VMEM((NY, 2, COL, PIECE, D), BF),
            pltpu.VMEM((NC, TOK, D), BF),
            pltpu.VMEM((NC, TOK, D), BF),
            pltpu.VMEM((D, TOKENS), BF),
            pltpu.VMEM((D, TOKENS), BF),
            pltpu.VMEM((NY, NB, TB, CH), F32),
            pltpu.VMEM((NY, NB, TB, CH), F32),
            pltpu.VMEM((NY, 1, CH), F32),
            pltpu.VMEM((CHIPS, NY, 2, 1, CH), F32),
            pltpu.VMEM((NY, D, CH), BF),
            pltpu.VMEM((NY, D, CH), BF),
            pltpu.VMEM((NY, D, CH), BF),
            pltpu.VMEM((NY, D, CH), BF),
            pltpu.VMEM((TOKENS, D), F32),
            pltpu.VMEM((TOKENS, D), F32),
            pltpu.VMEM((NX, 2, QT, D), BF),
            pltpu.VMEM((NX, 2, QT, D), BF),
            pltpu.VMEM((2, QT, D), BF),
            pltpu.VMEM((2, COL, PIECE, D), BF),
            pltpu.VMEM((COL, 2, PIECE, D), BF),
            dma((COL,)), dma((COL,)),
            dma((2,)), dma((2,)), dma((2,)),
            dma((2, 2, 4)), dma((2, 2, 4)),
            dma((NY,)), dma((NY,)), dma((NY,)), dma((NY,)),
            dma((CHIPS,)), dma((CHIPS,)),
            dma((NX,)), dma((NX,)),
            dma((COL,)), dma((COL,)),
            dma((NX,)), dma((2, 2)),
        ],
        compiler_params=pltpu.CompilerParams(
            collective_id=0, has_side_effects=True, vmem_limit_bytes=56 * 1024 * 1024
        ),
    )(xin, keys, values, nvis)
    out = fin.reshape(2, KV, ROWS, GROUP, D).transpose(0, 2, 1, 3, 4).reshape(2, ROWS, HEADS * D)
    grads = kvout.transpose(0, 1, 3, 2, 4).reshape(2, TOK, 2 * D)
    return out[0], out[1], grads[0], grads[1]


def solution(mesh):
    in_specs = (
        P(("mem", "kvh", "row"), None),
        P(("mem", "kvh", "row"), None),
        P("mem", "kvh"),
        P("mem", "kvh"),
        P(None, "row"),
        P(),
    )
    out_specs = (
        P(("mem", "kvh", "row"), None),
        P(("mem", "kvh", "row"), None),
        P("mem", "kvh"),
        P("mem", "kvh"),
    )
    return jax.shard_map(
        per_device, mesh=mesh, in_specs=in_specs, out_specs=out_specs, check_vma=False
    )
```

```python
import functools

import jax
import jax.numpy as jnp
from jax import lax
from jax.experimental import pallas as pl
from jax.experimental.pallas import tpu as pltpu
from jax.sharding import PartitionSpec as P

HEADS = 64
KV = 8
D = 128
GROUP = HEADS // KV
ROWS = 2
NY = 8
NZH = 2
NK = 4
NC = 2
NX = 4
COL = NZH * NK * NC
CHIPS = NZH * NY
PIECE = ROWS * GROUP
CH = COL * PIECE
TOK = 768
TOKENS = NC * TOK
TB = 384
NB = TOKENS // TB
QT = TOKENS // NX
FRAME = 128
SCALE = D ** (-0.5)
LOG2E = 1.4426950408889634
CS = SCALE * LOG2E
NEG = -1e30
MESH = pl.DeviceIdType.MESH
BF = jnp.bfloat16
F32 = jnp.float32


def dot_nt(a, b):
    return lax.dot_general(a, b, (((1,), (1,)), ((), ())), preferred_element_type=F32)


def dot_nn(a, b):
    return lax.dot_general(a, b, (((1,), (0,)), ((), ())), preferred_element_type=F32)


def kernel(
    xin, keys, values, nvis,
    fin_o, fin_q, kout, vout,
    buf, kbuf, vbuf, kt, vt, wbuf, dpbuf, dsbuf, mst, fst, dst, stats,
    osend, orecv, dqsend, dqrecv, dk, dv, rssend, rsrecv, agsrc, fsend, frecv,
    a_send, a_recv, kv_send, kv_recv, kv_loc, r_send, r_recv, o_send, o_recv, q_send, q_recv,
    s_send, s_recv, rs_send, rs_recv, f_send, f_recv, ag_send, ag_recv,
):
    m = lax.axis_index("mem")
    k = lax.axis_index("kvh")
    x = lax.axis_index("row")
    c = lax.rem(m, 2)
    n = lax.div(m, 2)
    y = lax.rem(n, NY)
    zh = lax.div(n, NY)
    s = (zh * NK + k) * NC + c

    def column(t):
        zz = lax.div(t, 2)
        return ((lax.div(zz, NK) * NY + y) * 2 + lax.rem(t, 2), lax.rem(zz, NK), x)

    def chip(t):
        return (t * 2 + c, k, x)

    def at_y(t):
        return ((zh * NY + t) * 2 + c, k, x)

    def at_x(t, core):
        return (n * 2 + core, k, t)

    def remote(src, dst, ss, rs, dev):
        return pltpu.make_async_remote_copy(
            src_ref=src, dst_ref=dst, send_sem=ss, recv_sem=rs, device_id=dev, device_id_type=MESH
        )

    other = 1 - c
    mine_cols = pl.ds(pl.multiple_of(c * D, D), D)
    other_cols = pl.ds(pl.multiple_of(other * D, D), D)
    loc_k = pltpu.make_async_copy(keys.at[:, mine_cols], kbuf.at[c], kv_loc.at[0])
    loc_v = pltpu.make_async_copy(values.at[:, mine_cols], vbuf.at[c], kv_loc.at[1])
    loc_k.start()
    loc_v.start()

    barrier = pltpu.get_barrier_semaphore()

    def greet_col(j, _):
        pl.semaphore_signal(barrier, inc=1, device_id=column(lax.rem(s + j, COL)), device_id_type=MESH)
        return 0

    def greet_chip(j, _):
        pl.semaphore_signal(barrier, inc=1, device_id=chip(lax.rem(n + j, CHIPS)), device_id_type=MESH)
        return 0

    lax.fori_loop(1, COL, greet_col, 0)
    lax.fori_loop(1, CHIPS, greet_chip, 0)
    for j in range(1, NX):
        for core in range(2):
            pl.semaphore_signal(
                barrier, inc=1, device_id=at_x(lax.rem(x + j, NX), core), device_id_type=MESH
            )
    pl.semaphore_wait(barrier, (COL - 1) + (CHIPS - 1) + 2 * (NX - 1))

    def a_copy(src_s, dst_s, dev):
        return remote(
            xin.at[lax.rem(dst_s, KV)], buf.at[y, :, src_s], a_send.at[dst_s], a_recv.at[src_s], dev
        )

    def a_start(j, _):
        t = lax.rem(s + j, COL)
        a_copy(s, t, column(t)).start()
        return 0

    lax.fori_loop(1, COL, a_start, 0)
    kcopy = remote(keys.at[:, other_cols], kbuf.at[c], kv_send.at[0], kv_recv.at[0], (n * 2 + other, k, x))
    vcopy = remote(values.at[:, other_cols], vbuf.at[c], kv_send.at[1], kv_recv.at[1], (n * 2 + other, k, x))
    kcopy.start()
    vcopy.start()
    own = xin[lax.rem(s, KV)]
    buf[y, 0, s] = own[0]
    buf[y, 1, s] = own[1]
    loc_k.wait()
    loc_v.wait()

    def a_wait(j, _):
        t = lax.rem(s + j, COL)
        a_copy(t, s, column(t)).wait_recv()
        return 0

    lax.fori_loop(1, COL, a_wait, 0)

    right = at_y(lax.rem(y + 1, NY))
    left = at_y(lax.rem(y + NY - 1, NY))

    def ring(way, kind, t):
        g = lax.rem(y + NY - t, NY) if way == 0 else lax.rem(y + t, NY)
        ref = buf.at[g, kind]
        return remote(ref, ref, r_send.at[way, kind, t], r_recv.at[way, kind, t], right if way == 0 else left)

    def ring_arrival(way, kind, t):
        g = lax.rem(y + NY - 1 - t, NY) if way == 0 else lax.rem(y + 1 + t, NY)
        ref = buf.at[g, kind]
        return remote(ref, ref, r_send.at[way, kind, t], r_recv.at[way, kind, t], right if way == 0 else left)

    for kind in range(2):
        for way in range(2):
            ring(way, kind, 0).start()

    kcopy.wait_recv()
    vcopy.wait_recv()
    for h in range(2):
        kt[:, h * TOK:(h + 1) * TOK] = kbuf[h].T
        vt[:, h * TOK:(h + 1) * TOK] = vbuf[h].T

    def chunk_at(i):
        half = lax.div(i + 1, 2)
        return jnp.where(lax.rem(i, 2) == 1, lax.rem(y + NY - half, NY), lax.rem(y + half, NY))

    def token_block(ref, b):
        h = b * TB // TOK
        return ref[h, b * TB - h * TOK:(b + 1) * TB - h * TOK]

    def stats_out(i):
        ref = stats.at[n, chunk_at(i)]

        def s_start(j, _):
            t = lax.rem(n + j, CHIPS)
            remote(ref, ref, s_send.at[t], s_recv.at[n], chip(t)).start()
            return 0

        lax.fori_loop(1, CHIPS, s_start, 0)

    def forward(i, _):
        @pl.when(lax.rem(i, 2) == 1)
        def _():
            t = lax.div(i - 1, 2)
            for kind in range(2):
                for way in range(2):
                    last_too = kind == way

                    if last_too:
                        ring_arrival(way, kind, t).wait_recv()

                        @pl.when(t < 3)
                        def _():
                            ring(way, kind, t + 1).start()
                    else:
                        @pl.when(t < 3)
                        def _():
                            ring_arrival(way, kind, t).wait_recv()

                        @pl.when(t < 2)
                        def _():
                            ring(way, kind, t + 1).start()

        @pl.when(i == 5)
        def _():
            def early(e, _):
                stats_out(e)
                return 0

            lax.fori_loop(0, 5, early, 0)

        g = chunk_at(i)
        q = buf[g, 0].reshape(CH, D)
        d = buf[g, 1].reshape(CH, D)
        nv = nvis[g]
        top = jnp.full((1, CH), NEG, F32)
        for b in range(NB):
            sc = dot_nt(token_block(kbuf, b), q)
            wbuf[g, b] = sc
            for u in range(TB // FRAME):
                part = jnp.max(sc[u * FRAME:(u + 1) * FRAME], axis=0, keepdims=True)
                top = jnp.maximum(top, jnp.where(nv > b * (TB // FRAME) + u, part, NEG))
        msc = top * CS
        total = jnp.zeros((1, CH), F32)
        dsum = jnp.zeros((1, CH), F32)
        acc = jnp.zeros((D, CH), F32)
        for b in range(NB):
            dp = dot_nt(token_block(vbuf, b), d)
            dpbuf[g, b] = dp
            ws = []
            for u in range(TB // FRAME):
                bias = jnp.where(nv > b * (TB // FRAME) + u, -msc, NEG)
                ws.append(jnp.exp2(wbuf[g, b, u * FRAME:(u + 1) * FRAME] * CS + bias))
            w = jnp.concatenate(ws, axis=0)
            wbuf[g, b] = w
            total = total + jnp.sum(w, axis=0, keepdims=True)
            dsum = dsum + jnp.sum(w * dp, axis=0, keepdims=True)
            acc = acc + dot_nn(vt[:, b * TB:(b + 1) * TB], w.astype(BF))
        seen = nv > 0
        inv = jnp.where(seen, 1.0 / jnp.where(seen, total, 1.0), 0.0)
        stats[n, g, 0] = jnp.where(seen, msc + jnp.log2(jnp.where(seen, total, 1.0)), NEG)
        stats[n, g, 1] = dsum * inv
        mst[g] = msc
        out = (acc * inv).astype(BF)

        osend[g] = out

        @pl.when(i >= 5)
        def _():
            stats_out(i)

        return 0

    lax.fori_loop(0, NY, forward, 0)

    def o_start(j, _):
        g = chunk_at(NY - 1 - j)
        remote(osend.at[g], orecv.at[y], o_send.at[g], o_recv.at[y], at_y(g)).start()
        return 0

    lax.fori_loop(0, NY - 1, o_start, 0)
    orecv[y] = osend[y]

    def s_wait(j, _):
        t = lax.rem(n + j, CHIPS)
        ref = stats.at[t]
        remote(ref, ref, s_send.at[t], s_recv.at[t], chip(t)).wait_recv()
        return 0

    lax.fori_loop(1, CHIPS, s_wait, 0)

    def whole_stats(g):
        peak = stats[0, g, 0]
        for t in range(1, CHIPS):
            peak = jnp.maximum(peak, stats[t, g, 0])
        mass = jnp.zeros((1, CH), F32)
        dsum = jnp.zeros((1, CH), F32)
        for t in range(CHIPS):
            e = jnp.exp2(stats[t, g, 0] - peak)
            mass = mass + e
            dsum = dsum + e * stats[t, g, 1]
        return peak + jnp.log2(mass), dsum / mass

    def prepare(g, _):
        lse, delta = whole_stats(g)
        fst[g] = jnp.exp2(mst[g] - lse)
        dst[g] = delta
        return 0

    lax.fori_loop(0, NY, prepare, 0)

    def rs_copy(src, to):
        return remote(rssend.at[to], rsrecv.at[src], rs_send.at[to], rs_recv.at[src], at_x(to, c))

    for j in (2, 1, 3, 0):
        b = lax.rem(x + j, NX)
        dk[...] = jnp.zeros_like(dk)
        dv[...] = jnp.zeros_like(dv)

        def quarter(g, _):
            q = buf[g, 0].reshape(CH, D)
            d = buf[g, 1].reshape(CH, D)
            f = fst[g]
            delta = dst[g]
            for u in range(QT // FRAME):
                rows = slice(u * FRAME, (u + 1) * FRAME)
                p = wbuf[g, b, rows] * f
                ds = (p * (dpbuf[g, b, rows] - delta)).astype(BF)
                dsbuf[g, b, rows] = ds
                dv[rows] = dv[rows] + dot_nn(p.astype(BF), d)
                dk[rows] = dk[rows] + dot_nn(ds, q)
            return 0

        lax.fori_loop(0, NY, quarter, 0)
        rssend[b, 0] = (dk[...] * SCALE).astype(BF)
        rssend[b, 1] = dv[...].astype(BF)
        if j:
            rs_copy(x, b).start()

    def query_chunk(i, _):
        g = chunk_at(NY - 1 - i)
        out = (dot_nn(kt[...], dsbuf[g].reshape(TOKENS, CH)) * SCALE).astype(BF)

        @pl.when(g == y)
        def _():
            dqrecv[y] = out

        @pl.when(g != y)
        def _():
            dqsend[g] = out
            remote(dqsend.at[g], dqrecv.at[y], q_send.at[g], q_recv.at[y], at_y(g)).start()

        return 0

    lax.fori_loop(0, NY, query_chunk, 0)

    def o_wait(j, _):
        t = lax.rem(y + j, NY)
        remote(osend.at[t], orecv.at[t], o_send.at[t], o_recv.at[t], at_y(t)).wait_recv()
        return 0

    lax.fori_loop(1, NY, o_wait, 0)
    lse, _ = whole_stats(y)
    acc = jnp.zeros((D, CH), F32)
    for t in range(NY):
        acc = acc + orecv[t].astype(F32) * jnp.exp2(stats[zh * NY + t, y, 0] - lse)
    fsend[0] = acc.T.astype(BF).reshape(COL, PIECE, D)

    for j in range(1, NX):
        rs_copy(lax.rem(x + j, NX), x).wait_recv()
    for a in range(2):
        acc = rssend[x, a].astype(F32)
        for j in range(1, NX):
            acc = acc + rsrecv[lax.rem(x + j, NX), a].astype(F32)
        agsrc[a] = acc.astype(BF)

    core = lax.div(x, 2)
    part = lax.rem(x, 2)
    grads = (kout, vout)

    def spot(ref, pp, hh):
        return ref.at[
            pl.ds(pl.multiple_of(pp * QT, QT), QT), pl.ds(pl.multiple_of(hh * D, D), D)
        ]

    def ag_copy(a, t):
        return remote(
            agsrc.at[a], spot(grads[a], part, c), ag_send.at[a, t], ag_recv.at[a, part, c], at_x(t, core)
        )

    for j in (2, 1, 3):
        for a in range(2):
            ag_copy(a, lax.rem(x + j, NX)).start()

    @pl.when(core != c)
    def _():
        ag_copy(0, x).start()
        ag_copy(1, x).start()

    @pl.when(core == c)
    def _():
        for a in range(2):
            spot(grads[a], part, c)[...] = agsrc[a]

    def q_wait(j, _):
        t = lax.rem(y + j, NY)
        remote(dqsend.at[t], dqrecv.at[t], q_send.at[t], q_recv.at[t], at_y(t)).wait_recv()
        return 0

    lax.fori_loop(1, NY, q_wait, 0)
    acc = jnp.zeros((D, CH), F32)
    for t in range(NY):
        acc = acc + dqrecv[t].astype(F32)
    fsend[1] = acc.T.astype(BF).reshape(COL, PIECE, D)

    def f_copy(src, dst):
        return remote(fsend.at[:, dst], frecv.at[src], f_send.at[dst], f_recv.at[src], column(dst))

    def f_start(j, _):
        f_copy(s, lax.rem(s + j, COL)).start()
        return 0

    lax.fori_loop(1, COL, f_start, 0)
    frecv[s, 0] = fsend[0, s]
    frecv[s, 1] = fsend[1, s]

    def f_wait(j, _):
        f_copy(lax.rem(s + j, COL), s).wait_recv()
        return 0

    lax.fori_loop(1, COL, f_wait, 0)
    for h in range(KV):
        fin_o[h] = (frecv[h, 0].astype(F32) + frecv[KV + h, 0].astype(F32)).astype(BF)
        fin_q[h] = (frecv[h, 1].astype(F32) + frecv[KV + h, 1].astype(F32)).astype(BF)

    for pp in range(2):
        for hh in range(2):
            itself = jnp.logical_and(c * 2 + pp == x, hh == c)

            @pl.when(jnp.logical_not(itself))
            def _():
                for a in range(2):
                    remote(
                        agsrc.at[a], spot(grads[a], pp, hh), ag_send.at[a, 0], ag_recv.at[a, pp, hh],
                        at_x(x, other),
                    ).wait_recv()

    def col_sent(j, _):
        t = lax.rem(s + j, COL)
        a_copy(s, t, column(t)).wait_send()
        f_copy(s, t).wait_send()
        return 0

    lax.fori_loop(1, COL, col_sent, 0)
    kcopy.wait_send()
    vcopy.wait_send()
    for kind in range(2):
        for way in range(2):
            for t in range(4 if kind == way else 3):
                ring(way, kind, t).wait_send()

    def y_sent(j, _):
        t = lax.rem(y + j, NY)
        remote(osend.at[t], orecv.at[y], o_send.at[t], o_recv.at[y], at_y(t)).wait_send()
        remote(dqsend.at[t], dqrecv.at[y], q_send.at[t], q_recv.at[y], at_y(t)).wait_send()
        return 0

    lax.fori_loop(1, NY, y_sent, 0)

    def s_sent(j, _):
        t = lax.rem(n + j, CHIPS)
        ref = stats.at[n]
        remote(ref, ref, s_send.at[t], s_recv.at[n], chip(t)).wait_send()
        return 0

    lax.fori_loop(1, CHIPS, s_sent, 0)
    for j in range(1, NX):
        rs_copy(x, lax.rem(x + j, NX)).wait_send()
        for a in range(2):
            ag_copy(a, lax.rem(x + j, NX)).wait_send()

    @pl.when(core != c)
    def _():
        ag_copy(0, x).wait_send()
        ag_copy(1, x).wait_send()


def per_device(queries, output_gradient, keys, values, text_video, video_blocks):
    n = lax.axis_index("mem") // 2
    both = jnp.stack([queries, output_gradient])
    xin = both.reshape(2, ROWS, KV, GROUP, D).transpose(2, 0, 1, 3, 4).reshape(KV, 2, PIECE, D)
    ids = jnp.arange(video_blocks.shape[0], dtype=jnp.int32)
    ends = jnp.sum(jnp.where(ids <= text_video[..., None], video_blocks, 0), axis=-1)
    frames = TOKENS // FRAME
    seen = jnp.clip(ends - n * frames, 0, frames)
    seen = seen.reshape(NZH, NY, NC, NK, ROWS).transpose(1, 0, 3, 2, 4)
    nvis = jnp.broadcast_to(seen[..., None], (NY, NZH, NK, NC, ROWS, GROUP)).reshape(NY, 1, CH)

    vm = pl.BlockSpec(memory_space=pltpu.VMEM)
    hbm = pl.BlockSpec(memory_space=pl.ANY)
    dma = pltpu.SemaphoreType.DMA
    fin_o, fin_q, key_grad, value_grad = pl.pallas_call(
        kernel,
        name="attention_step",
        out_shape=(
            jax.ShapeDtypeStruct((KV, PIECE, D), BF),
            jax.ShapeDtypeStruct((KV, PIECE, D), BF),
            jax.ShapeDtypeStruct((TOK, 2 * D), BF),
            jax.ShapeDtypeStruct((TOK, 2 * D), BF),
        ),
        in_specs=[vm, hbm, hbm, vm],
        out_specs=(vm, vm, vm, vm),
        scratch_shapes=[
            pltpu.VMEM((NY, 2, COL, PIECE, D), BF),
            pltpu.VMEM((NC, TOK, D), BF),
            pltpu.VMEM((NC, TOK, D), BF),
            pltpu.VMEM((D, TOKENS), BF),
            pltpu.VMEM((D, TOKENS), BF),
            pltpu.VMEM((NY, NB, TB, CH), F32),
            pltpu.VMEM((NY, NB, TB, CH), F32),
            pltpu.VMEM((NY, NB, TB, CH), BF),
            pltpu.VMEM((NY, 1, CH), F32),
            pltpu.VMEM((NY, 1, CH), F32),
            pltpu.VMEM((NY, 1, CH), F32),
            pltpu.VMEM((CHIPS, NY, 2, 1, CH), F32),
            pltpu.VMEM((NY, D, CH), BF),
            pltpu.VMEM((NY, D, CH), BF),
            pltpu.VMEM((NY, D, CH), BF),
            pltpu.VMEM((NY, D, CH), BF),
            pltpu.VMEM((QT, D), F32),
            pltpu.VMEM((QT, D), F32),
            pltpu.VMEM((NX, 2, QT, D), BF),
            pltpu.VMEM((NX, 2, QT, D), BF),
            pltpu.VMEM((2, QT, D), BF),
            pltpu.VMEM((2, COL, PIECE, D), BF),
            pltpu.VMEM((COL, 2, PIECE, D), BF),
            dma((COL,)), dma((COL,)),
            dma((2,)), dma((2,)), dma((2,)),
            dma((2, 2, 4)), dma((2, 2, 4)),
            dma((NY,)), dma((NY,)), dma((NY,)), dma((NY,)),
            dma((CHIPS,)), dma((CHIPS,)),
            dma((NX,)), dma((NX,)),
            dma((COL,)), dma((COL,)),
            dma((2, NX)), dma((2, 2, 2)),
        ],
        compiler_params=pltpu.CompilerParams(
            collective_id=0, has_side_effects=True, vmem_limit_bytes=56 * 1024 * 1024
        ),
    )(xin, keys, values, nvis)

    def flat(a):
        return a.reshape(KV, ROWS, GROUP, D).transpose(1, 0, 2, 3).reshape(ROWS, HEADS * D)

    return flat(fin_o), flat(fin_q), key_grad, value_grad


def solution(mesh):
    in_specs = (
        P(("mem", "kvh", "row"), None),
        P(("mem", "kvh", "row"), None),
        P("mem", "kvh"),
        P("mem", "kvh"),
        P(None, "row"),
        P(),
    )
    out_specs = (
        P(("mem", "kvh", "row"), None),
        P(("mem", "kvh", "row"), None),
        P("mem", "kvh"),
        P("mem", "kvh"),
    )
    return jax.shard_map(
        per_device, mesh=mesh, in_specs=in_specs, out_specs=out_specs, check_vma=False
    )
```

```python
import functools

import jax
import jax.numpy as jnp
from jax import lax
from jax.experimental import pallas as pl
from jax.experimental.pallas import tpu as pltpu
from jax.sharding import PartitionSpec as P

HEADS = 64
KV = 8
D = 128
GROUP = HEADS // KV
ROWS = 2
NY = 8
NZH = 2
NK = 4
NC = 2
NX = 4
COL = NZH * NK * NC
CHIPS = NZH * NY
PIECE = ROWS * GROUP
CH = COL * PIECE
TOK = 768
VIDEOS = 96
TOKENS = NC * TOK
TB = 384
NB = TOKENS // TB
QT = TOKENS // NX
FRAME = 128
SCALE = D ** (-0.5)
LOG2E = 1.4426950408889634
CS = SCALE * LOG2E
NEG = -1e30
MESH = pl.DeviceIdType.MESH
BF = jnp.bfloat16
F32 = jnp.float32


def dot_nt(a, b):
    return lax.dot_general(a, b, (((1,), (1,)), ((), ())), preferred_element_type=F32)


def dot_nn(a, b):
    return lax.dot_general(a, b, (((1,), (0,)), ((), ())), preferred_element_type=F32)


def kernel(
    xin, keys, values, last_seen, video_blocks,
    fin_o, fin_q, kout, vout,
    nvis, buf, kbuf, vbuf, kt, vt, wbuf, dpbuf, dsbuf, pbuf, mst, stats,
    osend, orecv, dqsend, dqrecv, dk, dv, rssend, rsrecv, agsrc, fsend, frecv,
    a_send, a_recv, kv_send, kv_recv, kv_loc, r_send, r_recv, o_send, o_recv, q_send, q_recv,
    s_send, s_recv, rs_send, rs_recv, f_send, f_recv, ag_send, ag_recv,
):
    m = lax.axis_index("mem")
    k = lax.axis_index("kvh")
    x = lax.axis_index("row")
    c = lax.rem(m, 2)
    n = lax.div(m, 2)
    y = lax.rem(n, NY)
    zh = lax.div(n, NY)
    s = (zh * NK + k) * NC + c

    def column(t):
        zz = lax.div(t, 2)
        return ((lax.div(zz, NK) * NY + y) * 2 + lax.rem(t, 2), lax.rem(zz, NK), x)

    def chip(t):
        return (t * 2 + c, k, x)

    def at_y(t):
        return ((zh * NY + t) * 2 + c, k, x)

    def at_x(t, core):
        return (n * 2 + core, k, t)

    def remote(src, dst, ss, rs, dev):
        return pltpu.make_async_remote_copy(
            src_ref=src, dst_ref=dst, send_sem=ss, recv_sem=rs, device_id=dev, device_id_type=MESH
        )

    other = 1 - c
    mine_cols = pl.ds(pl.multiple_of(c * D, D), D)
    other_cols = pl.ds(pl.multiple_of(other * D, D), D)
    loc_k = pltpu.make_async_copy(keys.at[:, mine_cols], kbuf.at[c], kv_loc.at[0])
    loc_v = pltpu.make_async_copy(values.at[:, mine_cols], vbuf.at[c], kv_loc.at[1])
    loc_k.start()
    loc_v.start()

    barrier = pltpu.get_barrier_semaphore()

    def greet_col(j, _):
        pl.semaphore_signal(barrier, inc=1, device_id=column(lax.rem(s + j, COL)), device_id_type=MESH)
        return 0

    def greet_chip(j, _):
        pl.semaphore_signal(barrier, inc=1, device_id=chip(lax.rem(n + j, CHIPS)), device_id_type=MESH)
        return 0

    lax.fori_loop(1, COL, greet_col, 0)
    lax.fori_loop(1, CHIPS, greet_chip, 0)
    for j in range(1, NX):
        for core in range(2):
            pl.semaphore_signal(
                barrier, inc=1, device_id=at_x(lax.rem(x + j, NX), core), device_id_type=MESH
            )

    seen_last = last_seen[...]
    ends = jnp.zeros(seen_last.shape, jnp.int32)
    for v in range(VIDEOS):
        ends = ends + jnp.where(seen_last >= v, video_blocks[v], 0)
    frames = TOKENS // FRAME
    counts = jnp.clip(ends - n * frames, 0, frames).astype(F32).astype(BF)
    lane = lax.broadcasted_iota(jnp.int32, (NZH * NY * NC * NK, CH), 1)
    group = lax.broadcasted_iota(jnp.int32, (NZH * NY * NC * NK, CH), 0)
    piece = lane // PIECE
    wanted = ((piece // (NK * NC)) * NY * NC + piece % NC) * NK + (piece // NC) % NK
    row = lax.broadcasted_iota(jnp.int32, (1, CH), 1) % ROWS
    for g in range(NY):
        pick = jnp.where(group == wanted + g * (NC * NK), 1.0, 0.0).astype(BF)
        both = dot_nn(counts, pick)
        nvis[g] = jnp.where(row == 0, both[0:1], both[1:2])

    pl.semaphore_wait(barrier, (COL - 1) + (CHIPS - 1) + 2 * (NX - 1))

    def a_copy(src_s, dst_s, dev):
        return remote(
            xin.at[lax.rem(dst_s, KV)], buf.at[y, :, src_s], a_send.at[dst_s], a_recv.at[src_s], dev
        )

    def a_start(j, _):
        t = lax.rem(s + j, COL)
        a_copy(s, t, column(t)).start()
        return 0

    lax.fori_loop(1, COL, a_start, 0)
    kcopy = remote(keys.at[:, other_cols], kbuf.at[c], kv_send.at[0], kv_recv.at[0], (n * 2 + other, k, x))
    vcopy = remote(values.at[:, other_cols], vbuf.at[c], kv_send.at[1], kv_recv.at[1], (n * 2 + other, k, x))
    kcopy.start()
    vcopy.start()
    own = xin[lax.rem(s, KV)]
    buf[y, 0, s] = own[0]
    buf[y, 1, s] = own[1]
    loc_k.wait()
    loc_v.wait()

    def a_wait(j, _):
        t = lax.rem(s + j, COL)
        a_copy(t, s, column(t)).wait_recv()
        return 0

    lax.fori_loop(1, COL, a_wait, 0)

    right = at_y(lax.rem(y + 1, NY))
    left = at_y(lax.rem(y + NY - 1, NY))

    def ring_piece(way, kind, h, t, g):
        ref = buf.at[g, kind, pl.ds(h * (COL // 2), COL // 2)]
        return remote(
            ref, ref, r_send.at[way, kind, h, t], r_recv.at[way, kind, h, t], right if way == 0 else left
        )

    def ring(way, kind, h, t):
        g = lax.rem(y + NY - t, NY) if way == 0 else lax.rem(y + t, NY)
        return ring_piece(way, kind, h, t, g)

    def ring_arrival(way, kind, h, t):
        g = lax.rem(y + NY - 1 - t, NY) if way == 0 else lax.rem(y + 1 + t, NY)
        return ring_piece(way, kind, h, t, g)

    pieces = [(way, kind, h) for kind in range(2) for h in range(2) for way in range(2)]
    for way, kind, h in pieces:
        ring(way, kind, h, 0).start()

    kcopy.wait_recv()
    vcopy.wait_recv()
    for h in range(2):
        kt[:, h * TOK:(h + 1) * TOK] = kbuf[h].T
        vt[:, h * TOK:(h + 1) * TOK] = vbuf[h].T

    def chunk_at(i):
        half = lax.div(i + 1, 2)
        return jnp.where(lax.rem(i, 2) == 1, lax.rem(y + NY - half, NY), lax.rem(y + half, NY))

    def token_block(ref, b):
        h = b * TB // TOK
        return ref[h, b * TB - h * TOK:(b + 1) * TB - h * TOK]

    def stats_out(first, count):
        ref = stats.at[n, pl.ds(first, count)]

        def s_start(j, _):
            t = lax.rem(n + j, CHIPS)
            remote(ref, ref, s_send.at[t], s_recv.at[n], chip(t)).start()
            return 0

        lax.fori_loop(1, CHIPS, s_start, 0)

    def forward(i, _):
        @pl.when(lax.rem(i, 2) == 1)
        def _():
            t = lax.div(i - 1, 2)
            for way, kind, h in pieces:
                if kind == way:
                    ring_arrival(way, kind, h, t).wait_recv()

                    @pl.when(t < 3)
                    def _():
                        ring(way, kind, h, t + 1).start()
                else:
                    @pl.when(t < 3)
                    def _():
                        ring_arrival(way, kind, h, t).wait_recv()

                    @pl.when(t < 2)
                    def _():
                        ring(way, kind, h, t + 1).start()

        @pl.when(i == 5)
        def _():
            stats_out(0, 5)

        g = chunk_at(i)
        q = buf[g, 0].reshape(CH, D)
        d = buf[g, 1].reshape(CH, D)
        nv = nvis[g]
        top = jnp.full((1, CH), NEG, F32)
        for b in range(NB):
            sc = dot_nt(token_block(kbuf, b), q)
            wbuf[g, b] = sc
            for u in range(TB // FRAME):
                part = jnp.max(sc[u * FRAME:(u + 1) * FRAME], axis=0, keepdims=True)
                top = jnp.maximum(top, jnp.where(nv > float(b * (TB // FRAME) + u), part, NEG))
        msc = top * CS
        total = jnp.zeros((1, CH), F32)
        dsum = jnp.zeros((1, CH), F32)
        acc = jnp.zeros((D, CH), F32)
        for b in range(NB):
            dp = dot_nt(token_block(vbuf, b), d)
            dpbuf[g, b] = dp
            ws = []
            for u in range(TB // FRAME):
                bias = jnp.where(nv > float(b * (TB // FRAME) + u), -msc, NEG)
                ws.append(jnp.exp2(wbuf[g, b, u * FRAME:(u + 1) * FRAME] * CS + bias))
            w = jnp.concatenate(ws, axis=0)
            wbuf[g, b] = w
            total = total + jnp.sum(w, axis=0, keepdims=True)
            dsum = dsum + jnp.sum(w * dp, axis=0, keepdims=True)
            acc = acc + dot_nn(vt[:, b * TB:(b + 1) * TB], w.astype(BF))
        seen = nv > 0.0
        inv = jnp.where(seen, 1.0 / jnp.where(seen, total, 1.0), 0.0)
        stats[n, i, 0] = jnp.where(seen, msc + jnp.log2(jnp.where(seen, total, 1.0)), NEG)
        stats[n, i, 1] = dsum * inv
        mst[g] = msc
        out = (acc * inv).astype(BF)

        osend[g] = out

        @pl.when(i == 6)
        def _():
            stats_out(5, 2)

        return 0

    lax.fori_loop(0, NY, forward, 0)
    stats_out(NY - 1, 1)

    def o_start(j, _):
        g = chunk_at(NY - 1 - j)
        remote(osend.at[g], orecv.at[y], o_send.at[g], o_recv.at[y], at_y(g)).start()
        return 0

    lax.fori_loop(0, NY - 1, o_start, 0)
    orecv[y] = osend[y]

    def s_wait(j, _):
        t = lax.rem(n + j, CHIPS)
        ref = stats.at[t]
        remote(ref, ref, s_send.at[t], s_recv.at[t], chip(t)).wait_recv()
        return 0

    lax.fori_loop(1, CHIPS, s_wait, 0)

    def order_at(t, g):
        r = lax.rem(g + NY - t % NY, NY)
        return jnp.where(r < 4, 2 * r, jnp.where(r == 4, NY - 1, 2 * NY - 1 - 2 * r))

    def whole_stats(g):
        at = [order_at(t, g) for t in range(NY)]
        tops = [stats[t, at[t % NY], 0] for t in range(CHIPS)]
        peak = functools.reduce(jnp.maximum, tops)
        mass = jnp.zeros((1, CH), F32)
        dsum = jnp.zeros((1, CH), F32)
        for t in range(CHIPS):
            e = jnp.exp2(tops[t] - peak)
            mass = mass + e
            dsum = dsum + e * stats[t, at[t % NY], 1]
        return peak + jnp.log2(mass), dsum / mass

    def query_chunk(i, _):
        g = chunk_at(NY - 1 - i)
        lse, delta = whole_stats(g)
        f = jnp.exp2(mst[g] - lse)
        acc = jnp.zeros((D, CH), F32)
        for b in range(NB):
            p = wbuf[g, b] * f
            ds = (p * (dpbuf[g, b] - delta)).astype(BF)
            pbuf[g, b] = p.astype(BF)
            dsbuf[g, b] = ds
            acc = acc + dot_nn(kt[:, b * TB:(b + 1) * TB], ds)
        out = (acc * SCALE).astype(BF)

        @pl.when(g == y)
        def _():
            dqrecv[y] = out

        @pl.when(g != y)
        def _():
            dqsend[g] = out
            remote(dqsend.at[g], dqrecv.at[y], q_send.at[g], q_recv.at[y], at_y(g)).start()

        return 0

    lax.fori_loop(0, NY, query_chunk, 0)

    def rs_copy(src, to):
        return remote(rssend.at[to], rsrecv.at[src], rs_send.at[to], rs_recv.at[src], at_x(to, c))

    def quarter(j, _):
        away = jnp.where(j == 0, 2, jnp.where(j == 1, 1, jnp.where(j == 2, 3, 0)))
        b = lax.rem(x + away, NX)
        for g in range(NY):
            part_v = dot_nn(pbuf[g, b], buf[g, 1].reshape(CH, D))
            part_k = dot_nn(dsbuf[g, b], buf[g, 0].reshape(CH, D))
            if g == 0:
                dv[...] = part_v
                dk[...] = part_k
            elif g < NY - 1:
                dv[...] = dv[...] + part_v
                dk[...] = dk[...] + part_k
            else:
                rssend[b, 1] = (dv[...] + part_v).astype(BF)
                rssend[b, 0] = ((dk[...] + part_k) * SCALE).astype(BF)

        @pl.when(j < NX - 1)
        def _():
            rs_copy(x, b).start()

        return 0

    lax.fori_loop(0, NX, quarter, 0)

    def o_wait(j, _):
        t = lax.rem(y + j, NY)
        remote(osend.at[t], orecv.at[t], o_send.at[t], o_recv.at[t], at_y(t)).wait_recv()
        return 0

    lax.fori_loop(1, NY, o_wait, 0)
    lse, _ = whole_stats(y)
    acc = jnp.zeros((D, CH), F32)
    for t in range(NY):
        acc = acc + orecv[t].astype(F32) * jnp.exp2(stats[zh * NY + t, order_at(t, y), 0] - lse)
    fsend[0] = acc.T.astype(BF).reshape(COL, PIECE, D)

    def f_copy(a, src, to):
        return remote(fsend.at[a, to], frecv.at[a, src], f_send.at[a, to], f_recv.at[a, src], column(to))

    def f_push(a):
        def start(j, _):
            f_copy(a, s, lax.rem(s + j, COL)).start()
            return 0

        lax.fori_loop(1, COL, start, 0)
        frecv[a, s] = fsend[a, s]

    f_push(0)

    for j in range(1, NX):
        rs_copy(lax.rem(x + j, NX), x).wait_recv()
    for a in range(2):
        acc = rssend[x, a].astype(F32)
        for j in range(1, NX):
            acc = acc + rsrecv[lax.rem(x + j, NX), a].astype(F32)
        agsrc[a] = acc.astype(BF)

    core = lax.div(x, 2)
    part = lax.rem(x, 2)
    grads = (kout, vout)

    def spot(ref, pp, hh):
        return ref.at[
            pl.ds(pl.multiple_of(pp * QT, QT), QT), pl.ds(pl.multiple_of(hh * D, D), D)
        ]

    def ag_copy(a, t):
        return remote(
            agsrc.at[a], spot(grads[a], part, c), ag_send.at[a, t], ag_recv.at[a, part, c], at_x(t, core)
        )

    for j in (2, 1, 3):
        for a in range(2):
            ag_copy(a, lax.rem(x + j, NX)).start()

    @pl.when(core != c)
    def _():
        ag_copy(0, x).start()
        ag_copy(1, x).start()

    @pl.when(core == c)
    def _():
        for a in range(2):
            spot(grads[a], part, c)[...] = agsrc[a]

    def q_wait(j, _):
        t = lax.rem(y + j, NY)
        remote(dqsend.at[t], dqrecv.at[t], q_send.at[t], q_recv.at[t], at_y(t)).wait_recv()
        return 0

    lax.fori_loop(1, NY, q_wait, 0)
    acc = jnp.zeros((D, CH), F32)
    for t in range(NY):
        acc = acc + dqrecv[t].astype(F32)
    fsend[1] = acc.T.astype(BF).reshape(COL, PIECE, D)

    f_push(1)

    def f_wait(j, _):
        f_copy(0, lax.rem(s + j, COL), s).wait_recv()
        f_copy(1, lax.rem(s + j, COL), s).wait_recv()
        return 0

    lax.fori_loop(1, COL, f_wait, 0)
    for h in range(KV):
        fin_o[h] = (frecv[0, h].astype(F32) + frecv[0, KV + h].astype(F32)).astype(BF)
        fin_q[h] = (frecv[1, h].astype(F32) + frecv[1, KV + h].astype(F32)).astype(BF)

    for pp in range(2):
        for hh in range(2):
            itself = jnp.logical_and(c * 2 + pp == x, hh == c)

            @pl.when(jnp.logical_not(itself))
            def _():
                for a in range(2):
                    remote(
                        agsrc.at[a], spot(grads[a], pp, hh), ag_send.at[a, 0], ag_recv.at[a, pp, hh],
                        at_x(x, other),
                    ).wait_recv()

    def col_sent(j, _):
        t = lax.rem(s + j, COL)
        a_copy(s, t, column(t)).wait_send()
        f_copy(0, s, t).wait_send()
        f_copy(1, s, t).wait_send()
        return 0

    lax.fori_loop(1, COL, col_sent, 0)
    kcopy.wait_send()
    vcopy.wait_send()
    for way, kind, h in pieces:
        for t in range(4 if kind == way else 3):
            ring(way, kind, h, t).wait_send()

    def y_sent(j, _):
        t = lax.rem(y + j, NY)
        remote(osend.at[t], orecv.at[y], o_send.at[t], o_recv.at[y], at_y(t)).wait_send()
        remote(dqsend.at[t], dqrecv.at[y], q_send.at[t], q_recv.at[y], at_y(t)).wait_send()
        return 0

    lax.fori_loop(1, NY, y_sent, 0)

    def s_sent(j, _):
        t = lax.rem(n + j, CHIPS)
        ref = stats.at[n]
        remote(ref, ref, s_send.at[t], s_recv.at[n], chip(t)).wait_send()
        return 0

    lax.fori_loop(1, CHIPS, s_sent, 0)
    for j in range(1, NX):
        rs_copy(x, lax.rem(x + j, NX)).wait_send()
        for a in range(2):
            ag_copy(a, lax.rem(x + j, NX)).wait_send()

    @pl.when(core != c)
    def _():
        ag_copy(0, x).wait_send()
        ag_copy(1, x).wait_send()


def per_device(queries, output_gradient, keys, values, text_video, video_blocks):
    both = jnp.stack([queries, output_gradient])
    xin = both.reshape(2, ROWS, KV, GROUP, D).transpose(2, 0, 3, 1, 4).reshape(KV, 2, PIECE, D)
    vm = pl.BlockSpec(memory_space=pltpu.VMEM)
    hbm = pl.BlockSpec(memory_space=pltpu.HBM)
    smem = pl.BlockSpec(memory_space=pltpu.SMEM)
    dma = pltpu.SemaphoreType.DMA
    fin_o, fin_q, key_grad, value_grad = pl.pallas_call(
        kernel,
        name="attention_step",
        out_shape=(
            jax.ShapeDtypeStruct((KV, PIECE, D), BF),
            jax.ShapeDtypeStruct((KV, PIECE, D), BF),
            jax.ShapeDtypeStruct((TOK, 2 * D), BF),
            jax.ShapeDtypeStruct((TOK, 2 * D), BF),
        ),
        in_specs=[vm, hbm, hbm, vm, smem],
        out_specs=(vm, vm, vm, vm),
        scratch_shapes=[
            pltpu.VMEM((NY, 1, CH), F32),
            pltpu.VMEM((NY, 2, COL, PIECE, D), BF),
            pltpu.VMEM((NC, TOK, D), BF),
            pltpu.VMEM((NC, TOK, D), BF),
            pltpu.VMEM((D, TOKENS), BF),
            pltpu.VMEM((D, TOKENS), BF),
            pltpu.VMEM((NY, NB, TB, CH), F32),
            pltpu.VMEM((NY, NB, TB, CH), F32),
            pltpu.VMEM((NY, NB, TB, CH), BF),
            pltpu.VMEM((NY, NB, TB, CH), BF),
            pltpu.VMEM((NY, 1, CH), F32),
            pltpu.VMEM((CHIPS, NY, 2, 1, CH), F32),
            pltpu.VMEM((NY, D, CH), BF),
            pltpu.VMEM((NY, D, CH), BF),
            pltpu.VMEM((NY, D, CH), BF),
            pltpu.VMEM((NY, D, CH), BF),
            pltpu.VMEM((QT, D), F32),
            pltpu.VMEM((QT, D), F32),
            pltpu.VMEM((NX, 2, QT, D), BF),
            pltpu.VMEM((NX, 2, QT, D), BF),
            pltpu.VMEM((2, QT, D), BF),
            pltpu.VMEM((2, COL, PIECE, D), BF),
            pltpu.VMEM((2, COL, PIECE, D), BF),
            dma((COL,)), dma((COL,)),
            dma((2,)), dma((2,)), dma((2,)),
            dma((2, 2, 2, 4)), dma((2, 2, 2, 4)),
            dma((NY,)), dma((NY,)), dma((NY,)), dma((NY,)),
            dma((CHIPS,)), dma((CHIPS,)),
            dma((NX,)), dma((NX,)),
            dma((2, COL)), dma((2, COL)),
            dma((2, NX)), dma((2, 2, 2)),
        ],
        compiler_params=pltpu.CompilerParams(
            collective_id=0, has_side_effects=True, vmem_limit_bytes=46 * 1024 * 1024
        ),
    )(
        xin,
        pltpu.with_memory_space_constraint(keys, pltpu.HBM),
        pltpu.with_memory_space_constraint(values, pltpu.HBM),
        text_video.T,
        video_blocks,
    )

    def flat(a):
        return a.reshape(KV, GROUP, ROWS, D).transpose(2, 0, 1, 3).reshape(ROWS, HEADS * D)

    return flat(fin_o), flat(fin_q), key_grad, value_grad


def solution(mesh):
    in_specs = (
        P(("mem", "kvh", "row"), None),
        P(("mem", "kvh", "row"), None),
        P("mem", "kvh"),
        P("mem", "kvh"),
        P(None, "row"),
        P(),
    )
    out_specs = (
        P(("mem", "kvh", "row"), None),
        P(("mem", "kvh", "row"), None),
        P("mem", "kvh"),
        P("mem", "kvh"),
    )
    return jax.shard_map(
        per_device, mesh=mesh, in_specs=in_specs, out_specs=out_specs, check_vma=False
    )
```

```python
import functools

import jax
import jax.numpy as jnp
from jax import lax
from jax.experimental import pallas as pl
from jax.experimental.pallas import tpu as pltpu
from jax.sharding import PartitionSpec as P

HEADS = 64
KV = 8
D = 128
GROUP = HEADS // KV
ROWS = 2
NY = 8
NZH = 2
NK = 4
NC = 2
NX = 4
COL = NZH * NK * NC
CHIPS = NZH * NY
PIECE = ROWS * GROUP
CH = COL * PIECE
TOK = 768
VIDEOS = 96
TOKENS = NC * TOK
TB = 384
NB = TOKENS // TB
QT = TOKENS // NX
FRAME = 128
SCALE = D ** (-0.5)
LOG2E = 1.4426950408889634
CS = SCALE * LOG2E
NEG = -1e30
MESH = pl.DeviceIdType.MESH
BF = jnp.bfloat16
F32 = jnp.float32


def dot_nt(a, b):
    return lax.dot_general(a, b, (((1,), (1,)), ((), ())), preferred_element_type=F32)


def dot_nn(a, b):
    return lax.dot_general(a, b, (((1,), (0,)), ((), ())), preferred_element_type=F32)


def kernel(
    queries, gradients, keys, values, last_seen_hbm, video_blocks_hbm,
    fin_o, fin_q, kout, vout,
    xin, last_seen, video_blocks, in_loc, nvis, buf, kbuf, vbuf, kt, vt, wbuf, dpbuf, dsbuf, pbuf, mst, stats,
    osend, orecv, dqsend, dqrecv, dk, dv, rssend, rsrecv, agsrc, fsend, frecv,
    a_send, a_recv, kv_send, kv_recv, kv_loc, r_send, r_recv, o_send, o_recv, q_send, q_recv,
    s_send, s_recv, rs_send, rs_recv, f_send, f_recv, ag_send, ag_recv,
):
    m = lax.axis_index("mem")
    k = lax.axis_index("kvh")
    x = lax.axis_index("row")
    c = lax.rem(m, 2)
    n = lax.div(m, 2)
    y = lax.rem(n, NY)
    zh = lax.div(n, NY)
    s = (zh * NK + k) * NC + c

    def column(t):
        zz = lax.div(t, 2)
        return ((lax.div(zz, NK) * NY + y) * 2 + lax.rem(t, 2), lax.rem(zz, NK), x)

    def chip(t):
        return (t * 2 + c, k, x)

    def at_y(t):
        return ((zh * NY + t) * 2 + c, k, x)

    def at_x(t, core):
        return (n * 2 + core, k, t)

    def remote(src, dst, ss, rs, dev):
        return pltpu.make_async_remote_copy(
            src_ref=src, dst_ref=dst, send_sem=ss, recv_sem=rs, device_id=dev, device_id_type=MESH
        )

    other = 1 - c
    mine_cols = pl.ds(pl.multiple_of(c * D, D), D)
    other_cols = pl.ds(pl.multiple_of(other * D, D), D)
    loc_k = pltpu.make_async_copy(keys.at[:, mine_cols], kbuf.at[c], kv_loc.at[0])
    loc_v = pltpu.make_async_copy(values.at[:, mine_cols], vbuf.at[c], kv_loc.at[1])
    into = [
        pltpu.make_async_copy(queries, xin.at[:, 0], in_loc.at[0]),
        pltpu.make_async_copy(gradients, xin.at[:, 1], in_loc.at[1]),
        pltpu.make_async_copy(last_seen_hbm, last_seen, in_loc.at[2]),
        pltpu.make_async_copy(video_blocks_hbm, video_blocks, in_loc.at[3]),
    ]
    for copy in into:
        copy.start()
    loc_k.start()
    loc_v.start()

    barrier = pltpu.get_barrier_semaphore()

    def greet_col(j, _):
        pl.semaphore_signal(barrier, inc=1, device_id=column(lax.rem(s + j, COL)), device_id_type=MESH)
        return 0

    def greet_chip(j, _):
        pl.semaphore_signal(barrier, inc=1, device_id=chip(lax.rem(n + j, CHIPS)), device_id_type=MESH)
        return 0

    lax.fori_loop(1, COL, greet_col, 0)
    lax.fori_loop(1, CHIPS, greet_chip, 0)
    for j in range(1, NX):
        for core in range(2):
            pl.semaphore_signal(
                barrier, inc=1, device_id=at_x(lax.rem(x + j, NX), core), device_id_type=MESH
            )

    for copy in into:
        copy.wait()
    seen_last = last_seen[...]
    ends = jnp.zeros(seen_last.shape, jnp.int32)
    for v in range(VIDEOS):
        ends = ends + jnp.where(seen_last >= v, video_blocks[v], 0)
    frames = TOKENS // FRAME
    counts = jnp.clip(ends - n * frames, 0, frames).astype(F32).astype(BF)
    lane = lax.broadcasted_iota(jnp.int32, (NZH * NY * NC * NK, CH), 1)
    group = lax.broadcasted_iota(jnp.int32, (NZH * NY * NC * NK, CH), 0)
    piece = lane // PIECE
    wanted = ((piece // (NK * NC)) * NY * NC + piece % NC) * NK + (piece // NC) % NK
    row = lax.broadcasted_iota(jnp.int32, (1, CH), 1) % ROWS
    for g in range(NY):
        pick = jnp.where(group == wanted + g * (NC * NK), 1.0, 0.0).astype(BF)
        both = dot_nn(counts, pick)
        nvis[g] = jnp.where(row == 0, both[0:1], both[1:2])

    pl.semaphore_wait(barrier, (COL - 1) + (CHIPS - 1) + 2 * (NX - 1))

    def a_copy(src_s, dst_s, dev):
        return remote(
            xin.at[lax.rem(dst_s, KV)], buf.at[y, :, src_s], a_send.at[dst_s], a_recv.at[src_s], dev
        )

    def a_start(j, _):
        t = lax.rem(s + j, COL)
        a_copy(s, t, column(t)).start()
        return 0

    lax.fori_loop(1, COL, a_start, 0)
    kcopy = remote(keys.at[:, other_cols], kbuf.at[c], kv_send.at[0], kv_recv.at[0], (n * 2 + other, k, x))
    vcopy = remote(values.at[:, other_cols], vbuf.at[c], kv_send.at[1], kv_recv.at[1], (n * 2 + other, k, x))
    kcopy.start()
    vcopy.start()
    own = xin[lax.rem(s, KV)]
    buf[y, 0, s] = own[0]
    buf[y, 1, s] = own[1]
    loc_k.wait()
    loc_v.wait()

    def a_wait(j, _):
        t = lax.rem(s + j, COL)
        a_copy(t, s, column(t)).wait_recv()
        return 0

    lax.fori_loop(1, COL, a_wait, 0)

    right = at_y(lax.rem(y + 1, NY))
    left = at_y(lax.rem(y + NY - 1, NY))

    def ring_piece(way, kind, h, t, g):
        ref = buf.at[g, kind, pl.ds(h * (COL // 2), COL // 2)]
        return remote(
            ref, ref, r_send.at[way, kind, h, t], r_recv.at[way, kind, h, t], right if way == 0 else left
        )

    def ring(way, kind, h, t):
        g = lax.rem(y + NY - t, NY) if way == 0 else lax.rem(y + t, NY)
        return ring_piece(way, kind, h, t, g)

    def ring_arrival(way, kind, h, t):
        g = lax.rem(y + NY - 1 - t, NY) if way == 0 else lax.rem(y + 1 + t, NY)
        return ring_piece(way, kind, h, t, g)

    pieces = [(way, kind, h) for kind in range(2) for h in range(2) for way in range(2)]
    for way, kind, h in pieces:
        ring(way, kind, h, 0).start()

    kcopy.wait_recv()
    vcopy.wait_recv()
    for h in range(2):
        kt[:, h * TOK:(h + 1) * TOK] = kbuf[h].T
        vt[:, h * TOK:(h + 1) * TOK] = vbuf[h].T

    def chunk_at(i):
        half = lax.div(i + 1, 2)
        return jnp.where(lax.rem(i, 2) == 1, lax.rem(y + NY - half, NY), lax.rem(y + half, NY))

    def token_block(ref, b):
        h = b * TB // TOK
        return ref[h, b * TB - h * TOK:(b + 1) * TB - h * TOK]

    def stats_out(first, count):
        ref = stats.at[n, pl.ds(first, count)]

        def s_start(j, _):
            t = lax.rem(n + j, CHIPS)
            remote(ref, ref, s_send.at[t], s_recv.at[n], chip(t)).start()
            return 0

        lax.fori_loop(1, CHIPS, s_start, 0)

    def forward(i, _):
        @pl.when(lax.rem(i, 2) == 1)
        def _():
            t = lax.div(i - 1, 2)
            for way, kind, h in pieces:
                if kind == way:
                    ring_arrival(way, kind, h, t).wait_recv()

                    @pl.when(t < 3)
                    def _():
                        ring(way, kind, h, t + 1).start()
                else:
                    @pl.when(t < 3)
                    def _():
                        ring_arrival(way, kind, h, t).wait_recv()

                    @pl.when(t < 2)
                    def _():
                        ring(way, kind, h, t + 1).start()

        @pl.when(i == 5)
        def _():
            stats_out(0, 5)

        g = chunk_at(i)
        q = buf[g, 0].reshape(CH, D)
        d = buf[g, 1].reshape(CH, D)
        nv = nvis[g]
        top = jnp.full((1, CH), NEG, F32)
        for b in range(NB):
            sc = dot_nt(token_block(kbuf, b), q)
            wbuf[g, b] = sc
            for u in range(TB // FRAME):
                part = jnp.max(sc[u * FRAME:(u + 1) * FRAME], axis=0, keepdims=True)
                top = jnp.maximum(top, jnp.where(nv > float(b * (TB // FRAME) + u), part, NEG))
        msc = top * CS
        total = jnp.zeros((1, CH), F32)
        dsum = jnp.zeros((1, CH), F32)
        acc = jnp.zeros((D, CH), F32)
        for b in range(NB):
            dp = dot_nt(token_block(vbuf, b), d)
            dpbuf[g, b] = dp
            ws = []
            for u in range(TB // FRAME):
                bias = jnp.where(nv > float(b * (TB // FRAME) + u), -msc, NEG)
                ws.append(jnp.exp2(wbuf[g, b, u * FRAME:(u + 1) * FRAME] * CS + bias))
            w = jnp.concatenate(ws, axis=0)
            wbuf[g, b] = w
            total = total + jnp.sum(w, axis=0, keepdims=True)
            dsum = dsum + jnp.sum(w * dp, axis=0, keepdims=True)
            acc = acc + dot_nn(vt[:, b * TB:(b + 1) * TB], w.astype(BF))
        seen = nv > 0.0
        inv = jnp.where(seen, 1.0 / jnp.where(seen, total, 1.0), 0.0)
        stats[n, i, 0] = jnp.where(seen, msc + jnp.log2(jnp.where(seen, total, 1.0)), NEG)
        stats[n, i, 1] = dsum * inv
        mst[g] = msc
        out = (acc * inv).astype(BF)

        osend[g] = out

        @pl.when(i == 6)
        def _():
            stats_out(5, 2)

        return 0

    lax.fori_loop(0, NY, forward, 0)
    stats_out(NY - 1, 1)

    def o_start(j, _):
        g = chunk_at(NY - 1 - j)
        remote(osend.at[g], orecv.at[y], o_send.at[g], o_recv.at[y], at_y(g)).start()
        return 0

    lax.fori_loop(0, NY - 1, o_start, 0)
    orecv[y] = osend[y]

    def s_wait(j, _):
        t = lax.rem(n + j, CHIPS)
        ref = stats.at[t]
        remote(ref, ref, s_send.at[t], s_recv.at[t], chip(t)).wait_recv()
        return 0

    lax.fori_loop(1, CHIPS, s_wait, 0)

    def order_at(t, g):
        r = lax.rem(g + NY - t % NY, NY)
        return jnp.where(r < 4, 2 * r, jnp.where(r == 4, NY - 1, 2 * NY - 1 - 2 * r))

    def whole_stats(g):
        at = [order_at(t, g) for t in range(NY)]
        tops = [stats[t, at[t % NY], 0] for t in range(CHIPS)]
        peak = functools.reduce(jnp.maximum, tops)
        mass = jnp.zeros((1, CH), F32)
        dsum = jnp.zeros((1, CH), F32)
        for t in range(CHIPS):
            e = jnp.exp2(tops[t] - peak)
            mass = mass + e
            dsum = dsum + e * stats[t, at[t % NY], 1]
        return peak + jnp.log2(mass), dsum / mass

    def query_chunk(i, _):
        g = chunk_at(NY - 1 - i)
        lse, delta = whole_stats(g)
        f = jnp.exp2(mst[g] - lse)
        acc = jnp.zeros((D, CH), F32)
        for b in range(NB):
            p = wbuf[g, b] * f
            ds = (p * (dpbuf[g, b] - delta)).astype(BF)
            pbuf[g, b] = p.astype(BF)
            dsbuf[g, b] = ds
            acc = acc + dot_nn(kt[:, b * TB:(b + 1) * TB], ds)
        out = (acc * SCALE).astype(BF)

        @pl.when(g == y)
        def _():
            dqrecv[y] = out

        @pl.when(g != y)
        def _():
            dqsend[g] = out
            remote(dqsend.at[g], dqrecv.at[y], q_send.at[g], q_recv.at[y], at_y(g)).start()

        return 0

    lax.fori_loop(0, NY, query_chunk, 0)

    def rs_copy(src, to):
        return remote(rssend.at[to], rsrecv.at[src], rs_send.at[to], rs_recv.at[src], at_x(to, c))

    def quarter(j, _):
        away = jnp.where(j == 0, 2, jnp.where(j == 1, 1, jnp.where(j == 2, 3, 0)))
        b = lax.rem(x + away, NX)
        for g in range(NY):
            part_v = dot_nn(pbuf[g, b], buf[g, 1].reshape(CH, D))
            part_k = dot_nn(dsbuf[g, b], buf[g, 0].reshape(CH, D))
            if g == 0:
                dv[...] = part_v
                dk[...] = part_k
            elif g < NY - 1:
                dv[...] = dv[...] + part_v
                dk[...] = dk[...] + part_k
            else:
                rssend[b, 1] = (dv[...] + part_v).astype(BF)
                rssend[b, 0] = ((dk[...] + part_k) * SCALE).astype(BF)

        @pl.when(j < NX - 1)
        def _():
            rs_copy(x, b).start()

        return 0

    lax.fori_loop(0, NX, quarter, 0)

    def o_wait(j, _):
        t = lax.rem(y + j, NY)
        remote(osend.at[t], orecv.at[t], o_send.at[t], o_recv.at[t], at_y(t)).wait_recv()
        return 0

    lax.fori_loop(1, NY, o_wait, 0)
    lse, _ = whole_stats(y)
    acc = jnp.zeros((D, CH), F32)
    for t in range(NY):
        acc = acc + orecv[t].astype(F32) * jnp.exp2(stats[zh * NY + t, order_at(t, y), 0] - lse)
    fsend[0] = acc.T.astype(BF).reshape(COL, PIECE, D)

    def f_copy(a, src, to):
        return remote(fsend.at[a, to], frecv.at[a, src], f_send.at[a, to], f_recv.at[a, src], column(to))

    def f_push(a):
        def start(j, _):
            f_copy(a, s, lax.rem(s + j, COL)).start()
            return 0

        lax.fori_loop(1, COL, start, 0)
        frecv[a, s] = fsend[a, s]

    f_push(0)

    for j in range(1, NX):
        rs_copy(lax.rem(x + j, NX), x).wait_recv()
    for a in range(2):
        acc = rssend[x, a].astype(F32)
        for j in range(1, NX):
            acc = acc + rsrecv[lax.rem(x + j, NX), a].astype(F32)
        agsrc[a] = acc.astype(BF)

    core = lax.div(x, 2)
    part = lax.rem(x, 2)
    grads = (kout, vout)

    def spot(ref, pp, hh):
        return ref.at[
            pl.ds(pl.multiple_of(pp * QT, QT), QT), pl.ds(pl.multiple_of(hh * D, D), D)
        ]

    def ag_copy(a, t):
        return remote(
            agsrc.at[a], spot(grads[a], part, c), ag_send.at[a, t], ag_recv.at[a, part, c], at_x(t, core)
        )

    for j in (2, 1, 3):
        for a in range(2):
            ag_copy(a, lax.rem(x + j, NX)).start()

    @pl.when(core != c)
    def _():
        ag_copy(0, x).start()
        ag_copy(1, x).start()

    @pl.when(core == c)
    def _():
        for a in range(2):
            spot(grads[a], part, c)[...] = agsrc[a]

    def q_wait(j, _):
        t = lax.rem(y + j, NY)
        remote(dqsend.at[t], dqrecv.at[t], q_send.at[t], q_recv.at[t], at_y(t)).wait_recv()
        return 0

    lax.fori_loop(1, NY, q_wait, 0)
    acc = jnp.zeros((D, CH), F32)
    for t in range(NY):
        acc = acc + dqrecv[t].astype(F32)
    fsend[1] = acc.T.astype(BF).reshape(COL, PIECE, D)

    f_push(1)

    def f_wait(j, _):
        f_copy(0, lax.rem(s + j, COL), s).wait_recv()
        f_copy(1, lax.rem(s + j, COL), s).wait_recv()
        return 0

    lax.fori_loop(1, COL, f_wait, 0)
    for h in range(KV):
        fin_o[h] = (frecv[0, h].astype(F32) + frecv[0, KV + h].astype(F32)).astype(BF)
        fin_q[h] = (frecv[1, h].astype(F32) + frecv[1, KV + h].astype(F32)).astype(BF)

    for pp in range(2):
        for hh in range(2):
            itself = jnp.logical_and(c * 2 + pp == x, hh == c)

            @pl.when(jnp.logical_not(itself))
            def _():
                for a in range(2):
                    remote(
                        agsrc.at[a], spot(grads[a], pp, hh), ag_send.at[a, 0], ag_recv.at[a, pp, hh],
                        at_x(x, other),
                    ).wait_recv()

    def col_sent(j, _):
        t = lax.rem(s + j, COL)
        a_copy(s, t, column(t)).wait_send()
        f_copy(0, s, t).wait_send()
        f_copy(1, s, t).wait_send()
        return 0

    lax.fori_loop(1, COL, col_sent, 0)
    kcopy.wait_send()
    vcopy.wait_send()
    for way, kind, h in pieces:
        for t in range(4 if kind == way else 3):
            ring(way, kind, h, t).wait_send()

    def y_sent(j, _):
        t = lax.rem(y + j, NY)
        remote(osend.at[t], orecv.at[y], o_send.at[t], o_recv.at[y], at_y(t)).wait_send()
        remote(dqsend.at[t], dqrecv.at[y], q_send.at[t], q_recv.at[y], at_y(t)).wait_send()
        return 0

    lax.fori_loop(1, NY, y_sent, 0)

    def s_sent(j, _):
        t = lax.rem(n + j, CHIPS)
        ref = stats.at[n]
        remote(ref, ref, s_send.at[t], s_recv.at[n], chip(t)).wait_send()
        return 0

    lax.fori_loop(1, CHIPS, s_sent, 0)
    for j in range(1, NX):
        rs_copy(x, lax.rem(x + j, NX)).wait_send()
        for a in range(2):
            ag_copy(a, lax.rem(x + j, NX)).wait_send()

    @pl.when(core != c)
    def _():
        ag_copy(0, x).wait_send()
        ag_copy(1, x).wait_send()


def per_device(queries, output_gradient, keys, values, text_video, video_blocks):
    def pieces(a):
        a = a.reshape(ROWS, KV, GROUP, D).transpose(1, 2, 0, 3).reshape(KV, PIECE, D)
        return pltpu.with_memory_space_constraint(a, pltpu.HBM)

    vm = pl.BlockSpec(memory_space=pltpu.VMEM)
    hbm = pl.BlockSpec(memory_space=pltpu.HBM)
    dma = pltpu.SemaphoreType.DMA
    fin_o, fin_q, key_grad, value_grad = pl.pallas_call(
        kernel,
        name="attention_step",
        out_shape=(
            jax.ShapeDtypeStruct((KV, PIECE, D), BF),
            jax.ShapeDtypeStruct((KV, PIECE, D), BF),
            jax.ShapeDtypeStruct((TOK, 2 * D), BF),
            jax.ShapeDtypeStruct((TOK, 2 * D), BF),
        ),
        in_specs=[hbm] * 6,
        out_specs=(vm, vm, vm, vm),
        scratch_shapes=[
            pltpu.VMEM((KV, 2, PIECE, D), BF),
            pltpu.VMEM((ROWS, NZH * NY * NC * NK), jnp.int32),
            pltpu.SMEM((VIDEOS,), jnp.int32),
            dma((4,)),
            pltpu.VMEM((NY, 1, CH), F32),
            pltpu.VMEM((NY, 2, COL, PIECE, D), BF),
            pltpu.VMEM((NC, TOK, D), BF),
            pltpu.VMEM((NC, TOK, D), BF),
            pltpu.VMEM((D, TOKENS), BF),
            pltpu.VMEM((D, TOKENS), BF),
            pltpu.VMEM((NY, NB, TB, CH), F32),
            pltpu.VMEM((NY, NB, TB, CH), F32),
            pltpu.VMEM((NY, NB, TB, CH), BF),
            pltpu.VMEM((NY, NB, TB, CH), BF),
            pltpu.VMEM((NY, 1, CH), F32),
            pltpu.VMEM((CHIPS, NY, 2, 1, CH), F32),
            pltpu.VMEM((NY, D, CH), BF),
            pltpu.VMEM((NY, D, CH), BF),
            pltpu.VMEM((NY, D, CH), BF),
            pltpu.VMEM((NY, D, CH), BF),
            pltpu.VMEM((QT, D), F32),
            pltpu.VMEM((QT, D), F32),
            pltpu.VMEM((NX, 2, QT, D), BF),
            pltpu.VMEM((NX, 2, QT, D), BF),
            pltpu.VMEM((2, QT, D), BF),
            pltpu.VMEM((2, COL, PIECE, D), BF),
            pltpu.VMEM((2, COL, PIECE, D), BF),
            dma((COL,)), dma((COL,)),
            dma((2,)), dma((2,)), dma((2,)),
            dma((2, 2, 2, 4)), dma((2, 2, 2, 4)),
            dma((NY,)), dma((NY,)), dma((NY,)), dma((NY,)),
            dma((CHIPS,)), dma((CHIPS,)),
            dma((NX,)), dma((NX,)),
            dma((2, COL)), dma((2, COL)),
            dma((2, NX)), dma((2, 2, 2)),
        ],
        compiler_params=pltpu.CompilerParams(
            collective_id=0, has_side_effects=True, vmem_limit_bytes=46 * 1024 * 1024
        ),
    )(
        pieces(queries),
        pieces(output_gradient),
        pltpu.with_memory_space_constraint(keys, pltpu.HBM),
        pltpu.with_memory_space_constraint(values, pltpu.HBM),
        pltpu.with_memory_space_constraint(text_video.T, pltpu.HBM),
        pltpu.with_memory_space_constraint(video_blocks, pltpu.HBM),
    )

    def flat(a):
        return a.reshape(KV, GROUP, ROWS, D).transpose(2, 0, 1, 3).reshape(ROWS, HEADS * D)

    return flat(fin_o), flat(fin_q), key_grad, value_grad


def solution(mesh):
    in_specs = (
        P(("mem", "kvh", "row"), None),
        P(("mem", "kvh", "row"), None),
        P("mem", "kvh"),
        P("mem", "kvh"),
        P(None, "row"),
        P(),
    )
    out_specs = (
        P(("mem", "kvh", "row"), None),
        P(("mem", "kvh", "row"), None),
        P("mem", "kvh"),
        P("mem", "kvh"),
    )
    return jax.shard_map(
        per_device, mesh=mesh, in_specs=in_specs, out_specs=out_specs, check_vma=False
    )
```
